32 devices in a mesh: groups: 2 (over y), blk: 4 (over z), desc: 2 (over x), half: 2 (over core).
Axes of the slice: x: 2, y: 2, z: 4, core: 2. Of those that a mesh axis runs over, the one named last changes fastest.
Arguments:
- descriptors: bfloat16 [8, 2048, 128], P(('groups', 'blk'), ('desc', 'half')), parts along dimension 0, may hold values from -0.5 to 0.5
Outputs:
- best_dist: float32 [3, 8, 2048], P(None, ('groups', 'blk'), 'desc'), parts along dimension 1
- second_dist: float32 [3, 8, 2048], P(None, ('groups', 'blk'), 'desc'), parts along dimension 1
The draws below stay inside these ranges and needn't reach their ends.
There are 2 independent parts, one for each index of `groups`. The reference program is written for one: setup_inputs(seed, part) draws one part's arguments, and reference() takes and returns one part's arrays. A program takes and returns all parts, laid end to end along the dimension named above; each array names one. Nothing has to cross between parts.
All inputs are finite; a program needn't handle non-finite values.
Results may differ from the reference program's by a relative error of at most 0.0003.
Values may be sent and summed in bfloat16 or wider, within the bound.
A program may use at most 64 MiB of HBM per device.

```python
import jax
import jax.numpy as jnp
from jax import lax

DESC = 2048
DIM = 128
IMAGES = 4


def block_levels(stream_key, extent, split, least, high):
    def one(position, parts):
        steps = jax.random.uniform(jax.random.fold_in(jax.random.fold_in(stream_key, 6), position), (parts,), jnp.float32, least / len(split), high / len(split))
        return jnp.repeat(jnp.exp(steps), extent[position] // parts).reshape((-1,) + (1,) * (len(extent) - position - 1))

    gain = one(*split[0])
    for cut in split[1:]:
        gain = gain * one(*cut)
    return gain


def bell_draw(own_key, extent, width, limit, shards=(), kind=jnp.bfloat16):
    values = jax.random.normal(own_key, extent, jnp.float32) * width
    if len(shards) > 0:
        values = block_levels(own_key, extent, shards, -0.22, 0.18) * values
    return jnp.clip(values, min=-limit, max=limit).astype(kind)


def setup_inputs(seed: int = 0, part: int = 0) -> dict:
    seeds = jax.random.split(jax.random.key(seed), 2)
    part_keys = jax.random.split(jax.random.fold_in(seeds[1], part), 2)
    descriptors = bell_draw(part_keys[0], (IMAGES, DESC, DIM), DIM ** -0.5, 0.5, ((0, 4), (1, 4)))
    return {"descriptors": descriptors}


def reference(descriptors):
    widened = descriptors.astype(jnp.float32)
    all_norms = jnp.sum(widened * widened, axis=2)

    def per_image(entry):
        image_rows, row_norms = entry
        products = jnp.einsum("rk,jck->jrc", image_rows, widened, precision=lax.Precision.HIGHEST)
        partial_value = all_norms[:, None, :] - 2.0 * products
        negated, unused = lax.top_k(-partial_value, 2)
        return row_norms[None, :] - negated[..., 0], row_norms[None, :] - negated[..., 1]

    best_all, second_all = lax.map(per_image, (widened, all_norms))
    query_index = jnp.arange(IMAGES, dtype=jnp.int32)
    offsets = jnp.arange(1, IMAGES, dtype=jnp.int32)
    cand_index = (query_index[None, :] - offsets[:, None]) % IMAGES
    best_dist = best_all[query_index[None, :], cand_index]
    second_dist = second_all[query_index[None, :], cand_index]
    return best_dist, second_dist
```

```python
import functools

import jax
import jax.numpy as jnp
from jax import lax
from jax.experimental import pallas as pl
from jax.experimental.pallas import tpu as pltpu
from jax.sharding import PartitionSpec as P

MESH = pl.DeviceIdType.MESH


def combine(lo_a, se_a, lo_b, se_b):
    return (
        jnp.minimum(lo_a, lo_b),
        jnp.minimum(jnp.maximum(lo_a, lo_b), jnp.minimum(se_a, se_b)),
    )


def nt_dot(a, b):
    return lax.dot_general(a, b, (((1,), (1,)), ((), ())), preferred_element_type=jnp.float32)


def kernel(
    n, D, H, CH, x_ref, best_ref, second_ref,
    buf, q, qn, low, sec, mine, inbox,
    z_send, z_recv, q_send, q_recv, p_send, p_recv,
):
    R = x_ref.shape[0]
    CR = R // CH
    share = H * R
    Q = D * share
    TQ = min(256, share)
    i = lax.axis_index("blk")
    d = lax.axis_index("desc")
    h = lax.axis_index("half")
    others = [(dd, hh) for dd in range(D) for hh in range(H) if (dd, hh) != (0, 0)]

    def peer(dd, hh):
        return {"desc": lax.rem(d + dd, D), "half": lax.rem(h + hh, H)}

    def rows_of(d_at, h_at):
        return pl.ds(pl.multiple_of((d_at * H + h_at) * R, R), R)

    def chunk(c):
        return pl.ds(pl.multiple_of(c * CR, CR), CR)

    def inside(j):
        return (j >= 0) & (j < n)

    barrier = pltpu.get_barrier_semaphore()
    for step in (1, -1):
        @pl.when(inside(i + step))
        def _():
            pl.semaphore_signal(barrier, inc=1, device_id={"blk": i + step}, device_id_type=MESH)
    for dd, hh in others:
        pl.semaphore_signal(barrier, inc=1, device_id=peer(dd, hh), device_id_type=MESH)
    links = jnp.where(inside(i + 1), 1, 0) + jnp.where(inside(i - 1), 1, 0)
    pl.semaphore_wait(barrier, len(others) + links)

    def own_copy(way, c):
        step = 1 - 2 * way
        return pltpu.make_async_remote_copy(
            src_ref=x_ref.at[chunk(c)], dst_ref=buf.at[i, chunk(c)],
            send_sem=z_send.at[way, i, c], recv_sem=z_recv.at[i, c],
            device_id={"blk": i + step}, device_id_type=MESH,
        )

    def relay_copy(way, j, c):
        step = 1 - 2 * way
        return pltpu.make_async_remote_copy(
            src_ref=buf.at[j, chunk(c)], dst_ref=buf.at[j, chunk(c)],
            send_sem=z_send.at[way, j, c], recv_sem=z_recv.at[j, c],
            device_id={"blk": i + step}, device_id_type=MESH,
        )

    for c in range(CH):
        for way in (0, 1):
            @pl.when(inside(i + 1 - 2 * way))
            def _():
                own_copy(way, c).start()

    mine_rows = rows_of(d, h)

    def query_copy(dd, hh):
        return pltpu.make_async_remote_copy(
            src_ref=x_ref, dst_ref=q.at[mine_rows],
            send_sem=q_send.at[dd * H + hh], recv_sem=q_recv.at[dd * H + hh],
            device_id=peer(dd, hh), device_id_type=MESH,
        )

    def query_relay(dd, hh):
        src_rows = rows_of(lax.rem(d + D - dd, D), h)
        return pltpu.make_async_remote_copy(
            src_ref=q.at[src_rows], dst_ref=q.at[src_rows],
            send_sem=q_send.at[dd * H + hh], recv_sem=q_recv.at[dd * H + hh],
            device_id=peer(0, hh), device_id_type=MESH,
        )

    for dd in range(1, D):
        query_copy(dd, 0).start()
    for hh in range(1, H):
        query_copy(0, hh).start()

    q[mine_rows, :] = x_ref[...]
    low[...] = jnp.full(low.shape, jnp.inf, jnp.float32)
    sec[...] = jnp.full(sec.shape, jnp.inf, jnp.float32)

    units = (n - 1) * CH * 2
    ahead = CH * 2

    def place(u):
        way = lax.rem(u, 2)
        c = lax.rem(lax.div(u, 2), CH)
        s = lax.div(u, 2 * CH) + 1
        j = jnp.where(way == 0, i - s, i + s)
        return way, c, s, j

    def relay(u):
        way, c, s, j = place(u)

        @pl.when(inside(j) & inside(i + 1 - 2 * way) & (u < units))
        def _():
            copy = relay_copy(way, j, c)
            copy.wait_recv()
            copy.start()

    def relays(u, carry):
        relay(u)
        return carry

    lax.fori_loop(0, ahead, relays, 0)

    for dd in range(1, D):
        query_copy(dd, 0).wait_recv()
        for hh in range(1, H):
            query_relay(dd, hh).start()
    for dd in range(D):
        for hh in range(1, H):
            query_copy(dd, hh).wait_recv()

    ones = jnp.ones((8, q.shape[1]), jnp.bfloat16)
    for t in range(D):
        wide = q[t * share : (t + 1) * share, :].astype(jnp.float32)
        square = wide * wide
        head = square.astype(jnp.bfloat16)
        tail = (square - head.astype(jnp.float32)).astype(jnp.bfloat16)
        qn[t] = nt_dot(ones, head) + nt_dot(ones, tail)

    def result_copy(k, dd, hh):
        return pltpu.make_async_remote_copy(
            src_ref=mine.at[k, lax.rem(d + dd, D)], dst_ref=inbox.at[k, dd * H + hh],
            send_sem=p_send.at[k, dd * H + hh], recv_sem=p_recv.at[k, dd * H + hh],
            device_id=peer(dd, hh), device_id_type=MESH,
        )

    def work(u, carry):
        relay(u + ahead)
        way, c, s, j = place(u)

        @pl.when(inside(j))
        def _():
            @pl.when(jnp.logical_not(inside(i + 1 - 2 * way)))
            def _():
                relay_copy(way, j, c).wait_recv()

            k = jnp.where(way == 0, s, n - s) - 1
            piece = buf[j, chunk(c), :]
            wide = piece.astype(jnp.float32)
            norms = jnp.sum(wide * wide, axis=1, keepdims=True)
            scaled = (wide * -2.0).astype(jnp.bfloat16)
            for t in range(Q // TQ):
                lanes = slice(t * TQ, (t + 1) * TQ)
                part = nt_dot(scaled, q[lanes, :]) + norms
                lo, se = low[k, :, lanes], sec[k, :, lanes]
                for r in range(CR // 8):
                    value = part[8 * r : 8 * r + 8]
                    se = jnp.minimum(se, jnp.maximum(lo, value))
                    lo = jnp.minimum(lo, value)
                low[k, :, lanes] = lo
                sec[k, :, lanes] = se

            @pl.when(c == CH - 1)
            def _():
                for t in range(D):
                    lanes = slice(t * share, (t + 1) * share)
                    lo, se = low[k, :, lanes], sec[k, :, lanes]
                    for turn in (4, 2, 1):
                        lo, se = combine(
                            lo, se, pltpu.roll(lo, turn, 0), pltpu.roll(se, turn, 0)
                        )
                    mine[k, t, 0:1, :] = lo[0:1]
                    mine[k, t, 1:2, :] = se[0:1]
                for dd, hh in reversed(others):
                    result_copy(k, dd, hh).start()

        return carry

    lax.fori_loop(0, units, work, 0)

    def finish(k, carry):
        lo, se = mine[k, d, 0:1, :], mine[k, d, 1:2, :]
        for dd, hh in others:
            result_copy(k, dd, hh).wait_recv()
            at = dd * H + hh
            lo, se = combine(lo, se, inbox[k, at, 0:1, :], inbox[k, at, 1:2, :])
        norms = qn[d, 0:1, :]
        best_ref[k] = norms + lo
        second_ref[k] = norms + se
        return carry

    lax.fori_loop(0, n - 1, finish, 0)

    def sent_results(k, carry):
        for dd, hh in others:
            result_copy(k, dd, hh).wait_send()
        return carry

    lax.fori_loop(0, n - 1, sent_results, 0)

    def sent_relays(u, carry):
        way, c, s, j = place(u)

        @pl.when(inside(j) & inside(i + 1 - 2 * way))
        def _():
            relay_copy(way, j, c).wait_send()

        return carry

    lax.fori_loop(0, units, sent_relays, 0)
    for c in range(CH):
        for way in (0, 1):
            @pl.when(inside(i + 1 - 2 * way))
            def _():
                own_copy(way, c).wait_send()
    for dd in range(1, D):
        query_copy(dd, 0).wait_send()
        for hh in range(1, H):
            query_relay(dd, hh).wait_send()
    for hh in range(1, H):
        query_copy(0, hh).wait_send()


def solution(mesh):
    n, D, H = mesh.shape["blk"], mesh.shape["desc"], mesh.shape["half"]

    def per_device(descriptors):
        block = descriptors[0]
        R, depth = block.shape
        CH = 2 if R % 32 == 0 else 1
        share = H * R
        out = jax.ShapeDtypeStruct((n - 1, 1, share), jnp.float32)
        vmem = pl.BlockSpec(memory_space=pltpu.VMEM)
        return pl.pallas_call(
            functools.partial(kernel, n, D, H, CH),
            out_shape=(out, out),
            in_specs=[vmem],
            out_specs=(vmem, vmem),
            scratch_shapes=[
                pltpu.VMEM((n, R, depth), jnp.bfloat16),
                pltpu.VMEM((D * share, depth), jnp.bfloat16),
                pltpu.VMEM((D, 8, share), jnp.float32),
                pltpu.VMEM((n - 1, 8, D * share), jnp.float32),
                pltpu.VMEM((n - 1, 8, D * share), jnp.float32),
                pltpu.VMEM((n - 1, D, 2, share), jnp.float32),
                pltpu.VMEM((n - 1, D * H, 2, share), jnp.float32),
                pltpu.SemaphoreType.DMA((2, n, CH)),
                pltpu.SemaphoreType.DMA((n, CH)),
                pltpu.SemaphoreType.DMA((D * H,)),
                pltpu.SemaphoreType.DMA((D * H,)),
                pltpu.SemaphoreType.DMA((n - 1, D * H)),
                pltpu.SemaphoreType.DMA((n - 1, D * H)),
            ],
            compiler_params=pltpu.CompilerParams(collective_id=0, has_side_effects=True),
        )(block)

    in_specs = (P(("groups", "blk"), ("desc", "half"), None),)
    out_specs = (P(None, ("groups", "blk"), "desc"), P(None, ("groups", "blk"), "desc"))
    return jax.shard_map(
        per_device, mesh=mesh, in_specs=in_specs, out_specs=out_specs, check_vma=False
    )
```

```python
import functools

import jax
import jax.numpy as jnp
from jax import lax
from jax.experimental import pallas as pl
from jax.experimental.pallas import tpu as pltpu
from jax.sharding import PartitionSpec as P

MESH = pl.DeviceIdType.MESH


def combine(lo_a, se_a, lo_b, se_b):
    return (
        jnp.minimum(lo_a, lo_b),
        jnp.minimum(jnp.maximum(lo_a, lo_b), jnp.minimum(se_a, se_b)),
    )


def nt_dot(a, b):
    return lax.dot_general(a, b, (((1,), (1,)), ((), ())), preferred_element_type=jnp.float32)


def kernel(
    n, D, H, CH, x_hbm, best_ref, second_ref, norm_ref,
    x_ref, buf, q, qn, low, sec, mine, inbox,
    x_sem, z_send, z_recv, q_send, q_recv, p_send, p_recv,
):
    R = x_hbm.shape[0]
    load = pltpu.make_async_copy(x_hbm, x_ref, x_sem)
    load.start()
    CR = R // CH
    share = H * R
    Q = D * share
    TQ = min(256, share)
    i = lax.axis_index("blk")
    d = lax.axis_index("desc")
    h = lax.axis_index("half")
    others = [(dd, hh) for dd in range(D) for hh in range(H) if (dd, hh) != (0, 0)]

    def peer(dd, hh):
        return {"desc": lax.rem(d + dd, D), "half": lax.rem(h + hh, H)}

    def rows_of(d_at, h_at):
        return pl.ds(pl.multiple_of((d_at * H + h_at) * R, R), R)

    def chunk(c):
        return pl.ds(pl.multiple_of(c * CR, CR), CR)

    def inside(j):
        return (j >= 0) & (j < n)

    barrier = pltpu.get_barrier_semaphore()
    for step in (1, -1):
        @pl.when(inside(i + step))
        def _():
            pl.semaphore_signal(barrier, inc=1, device_id={"blk": i + step}, device_id_type=MESH)
    for dd, hh in others:
        pl.semaphore_signal(barrier, inc=1, device_id=peer(dd, hh), device_id_type=MESH)
    links = jnp.where(inside(i + 1), 1, 0) + jnp.where(inside(i - 1), 1, 0)
    low[...] = jnp.full(low.shape, jnp.inf, jnp.float32)
    sec[...] = jnp.full(sec.shape, jnp.inf, jnp.float32)
    load.wait()
    pl.semaphore_wait(barrier, len(others) + links)

    def own_copy(way, c):
        step = 1 - 2 * way
        return pltpu.make_async_remote_copy(
            src_ref=x_ref.at[chunk(c)], dst_ref=buf.at[i, chunk(c)],
            send_sem=z_send.at[way, i, c], recv_sem=z_recv.at[i, c],
            device_id={"blk": i + step}, device_id_type=MESH,
        )

    def relay_copy(way, j, c):
        step = 1 - 2 * way
        return pltpu.make_async_remote_copy(
            src_ref=buf.at[j, chunk(c)], dst_ref=buf.at[j, chunk(c)],
            send_sem=z_send.at[way, j, c], recv_sem=z_recv.at[j, c],
            device_id={"blk": i + step}, device_id_type=MESH,
        )

    for c in range(CH):
        for way in (0, 1):
            @pl.when(inside(i + 1 - 2 * way))
            def _():
                own_copy(way, c).start()

    mine_rows = rows_of(d, h)

    def query_copy(dd, hh):
        return pltpu.make_async_remote_copy(
            src_ref=x_ref, dst_ref=q.at[mine_rows],
            send_sem=q_send.at[dd * H + hh], recv_sem=q_recv.at[dd * H + hh],
            device_id=peer(dd, hh), device_id_type=MESH,
        )

    def query_relay(dd, hh):
        src_rows = rows_of(lax.rem(d + D - dd, D), h)
        return pltpu.make_async_remote_copy(
            src_ref=q.at[src_rows], dst_ref=q.at[src_rows],
            send_sem=q_send.at[dd * H + hh], recv_sem=q_recv.at[dd * H + hh],
            device_id=peer(0, hh), device_id_type=MESH,
        )

    for dd in range(1, D):
        query_copy(dd, 0).start()
    for hh in range(1, H):
        query_copy(0, hh).start()

    q[mine_rows, :] = x_ref[...]

    units = (n - 1) * CH * 2
    ahead = CH * 2

    def place(u):
        way = lax.rem(u, 2)
        c = lax.rem(lax.div(u, 2), CH)
        s = lax.div(u, 2 * CH) + 1
        j = jnp.where(way == 0, i - s, i + s)
        return way, c, s, j

    def relay(u):
        way, c, s, j = place(u)

        @pl.when(inside(j) & inside(i + 1 - 2 * way) & (u < units))
        def _():
            copy = relay_copy(way, j, c)
            copy.wait_recv()
            copy.start()

    def relays(u, carry):
        relay(u)
        return carry

    lax.fori_loop(0, ahead, relays, 0)

    for dd in range(1, D):
        query_copy(dd, 0).wait_recv()
        for hh in range(1, H):
            query_relay(dd, hh).start()
    for dd in range(D):
        for hh in range(1, H):
            query_copy(dd, hh).wait_recv()

    ones = jnp.ones((8, q.shape[1]), jnp.bfloat16)
    for t in range(D):
        wide = q[t * share : (t + 1) * share, :].astype(jnp.float32)
        square = wide * wide
        head = square.astype(jnp.bfloat16)
        tail = (square - head.astype(jnp.float32)).astype(jnp.bfloat16)
        qn[t] = nt_dot(ones, head) + nt_dot(ones, tail)

    def result_copy(k, dd, hh):
        return pltpu.make_async_remote_copy(
            src_ref=mine.at[k, lax.rem(d + dd, D)], dst_ref=inbox.at[k, dd * H + hh],
            send_sem=p_send.at[k, dd * H + hh], recv_sem=p_recv.at[k, dd * H + hh],
            device_id=peer(dd, hh), device_id_type=MESH,
        )

    def work(u, carry):
        relay(u + ahead)
        way, c, s, j = place(u)

        @pl.when(inside(j))
        def _():
            @pl.when(jnp.logical_not(inside(i + 1 - 2 * way)))
            def _():
                relay_copy(way, j, c).wait_recv()

            k = jnp.where(way == 0, s, n - s) - 1
            piece = buf[j, chunk(c), :]
            wide = piece.astype(jnp.float32)
            norms = jnp.sum(wide * wide, axis=1, keepdims=True)
            scaled = (wide * -2.0).astype(jnp.bfloat16)
            for t in range(Q // TQ):
                lanes = slice(t * TQ, (t + 1) * TQ)
                part = nt_dot(scaled, q[lanes, :]) + norms
                lo, se = low[k, :, lanes], sec[k, :, lanes]
                for r in range(CR // 8):
                    value = part[8 * r : 8 * r + 8]
                    se = jnp.minimum(se, jnp.maximum(lo, value))
                    lo = jnp.minimum(lo, value)
                low[k, :, lanes] = lo
                sec[k, :, lanes] = se

            @pl.when(c == CH - 1)
            def _():
                for t in range(D):
                    lanes = slice(t * share, (t + 1) * share)
                    lo, se = low[k, :, lanes], sec[k, :, lanes]
                    for turn in (4, 2, 1):
                        lo, se = combine(
                            lo, se, pltpu.roll(lo, turn, 0), pltpu.roll(se, turn, 0)
                        )
                    mine[k, t, 0:1, :] = lo[0:1]
                    mine[k, t, 1:2, :] = se[0:1]
                for dd, hh in reversed(others):
                    result_copy(k, dd, hh).start()

        return carry

    lax.fori_loop(0, units, work, 0)

    def finish(k, carry):
        lo, se = mine[k, d, 0:1, :], mine[k, d, 1:2, :]
        for dd, hh in others:
            result_copy(k, dd, hh).wait_recv()
            at = dd * H + hh
            lo, se = combine(lo, se, inbox[k, at, 0:1, :], inbox[k, at, 1:2, :])
        norms = qn[d, 0:1, :]
        best_ref[k] = lo
        second_ref[k] = se
        norm_ref[...] = norms
        return carry

    lax.fori_loop(0, n - 1, finish, 0)

    def sent_results(k, carry):
        for dd, hh in others:
            result_copy(k, dd, hh).wait_send()
        return carry

    lax.fori_loop(0, n - 1, sent_results, 0)

    def sent_relays(u, carry):
        way, c, s, j = place(u)

        @pl.when(inside(j) & inside(i + 1 - 2 * way))
        def _():
            relay_copy(way, j, c).wait_send()

        return carry

    lax.fori_loop(0, units, sent_relays, 0)
    for c in range(CH):
        for way in (0, 1):
            @pl.when(inside(i + 1 - 2 * way))
            def _():
                own_copy(way, c).wait_send()
    for dd in range(1, D):
        query_copy(dd, 0).wait_send()
        for hh in range(1, H):
            query_relay(dd, hh).wait_send()
    for hh in range(1, H):
        query_copy(0, hh).wait_send()


def solution(mesh):
    n, D, H = mesh.shape["blk"], mesh.shape["desc"], mesh.shape["half"]

    def per_device(descriptors):
        block = descriptors[0]
        R, depth = block.shape
        CH = 2 if R % 32 == 0 else 1
        share = H * R
        out = pltpu.VMEM((n - 1, 1, share), jnp.float32)
        vmem = pl.BlockSpec(memory_space=pltpu.VMEM)
        lo, se, norms = pl.pallas_call(
            functools.partial(kernel, n, D, H, CH),
            out_shape=(out, out, pltpu.VMEM((1, share), jnp.float32)),
            in_specs=[pl.BlockSpec(memory_space=pltpu.HBM)],
            out_specs=(vmem, vmem, vmem),
            scratch_shapes=[
                pltpu.VMEM((R, depth), jnp.bfloat16),
                pltpu.VMEM((n, R, depth), jnp.bfloat16),
                pltpu.VMEM((D * share, depth), jnp.bfloat16),
                pltpu.VMEM((D, 8, share), jnp.float32),
                pltpu.VMEM((n - 1, 8, D * share), jnp.float32),
                pltpu.VMEM((n - 1, 8, D * share), jnp.float32),
                pltpu.VMEM((n - 1, D, 2, share), jnp.float32),
                pltpu.VMEM((n - 1, D * H, 2, share), jnp.float32),
                pltpu.SemaphoreType.DMA,
                pltpu.SemaphoreType.DMA((2, n, CH)),
                pltpu.SemaphoreType.DMA((n, CH)),
                pltpu.SemaphoreType.DMA((D * H,)),
                pltpu.SemaphoreType.DMA((D * H,)),
                pltpu.SemaphoreType.DMA((n - 1, D * H)),
                pltpu.SemaphoreType.DMA((n - 1, D * H)),
            ],
            compiler_params=pltpu.CompilerParams(collective_id=0, has_side_effects=True),
        )(block)
        return norms + lo, norms + se

    in_specs = (P(("groups", "blk"), ("desc", "half"), None),)
    out_specs = (P(None, ("groups", "blk"), "desc"), P(None, ("groups", "blk"), "desc"))
    return jax.shard_map(
        per_device, mesh=mesh, in_specs=in_specs, out_specs=out_specs, check_vma=False
    )
```

```python
import functools

import jax
import jax.numpy as jnp
from jax import lax
from jax.experimental import pallas as pl
from jax.experimental.pallas import tpu as pltpu
from jax.sharding import PartitionSpec as P

MESH = pl.DeviceIdType.MESH


def combine(lo_a, se_a, lo_b, se_b):
    return (
        jnp.minimum(lo_a, lo_b),
        jnp.minimum(jnp.maximum(lo_a, lo_b), jnp.minimum(se_a, se_b)),
    )


def nt_dot(a, b):
    return lax.dot_general(a, b, (((1,), (1,)), ((), ())), preferred_element_type=jnp.float32)


def kernel(
    n, D, H, CH, x_hbm, best_ref, second_ref, norm_ref,
    x_ref, buf, q, qn, low, sec, mine, inbox,
    x_sem, f_send, z_send, z_recv, q_send, q_recv, p_send, p_recv,
):
    R = x_hbm.shape[0]
    load = pltpu.make_async_copy(x_hbm, x_ref, x_sem)
    load.start()
    CR = R // CH
    share = H * R
    Q = D * share
    TQ = min(256, share)
    i = lax.axis_index("blk")
    d = lax.axis_index("desc")
    h = lax.axis_index("half")
    others = [(dd, hh) for dd in range(D) for hh in range(H) if (dd, hh) != (0, 0)]

    def peer(dd, hh):
        return {"desc": lax.rem(d + dd, D), "half": lax.rem(h + hh, H)}

    def rows_of(d_at, h_at):
        return pl.ds(pl.multiple_of((d_at * H + h_at) * R, R), R)

    def chunk(c):
        return pl.ds(pl.multiple_of(c * CR, CR), CR)

    def inside(j):
        return (j >= 0) & (j < n)

    barrier = pltpu.get_barrier_semaphore()
    for step in (1, -1):
        @pl.when(inside(i + step))
        def _():
            pl.semaphore_signal(barrier, inc=1, device_id={"blk": i + step}, device_id_type=MESH)
    for dd, hh in others:
        pl.semaphore_signal(barrier, inc=1, device_id=peer(dd, hh), device_id_type=MESH)
    at_end = ((i == 0) | (i == n - 1)) & (n > 2)
    opposite = n - 1 - i

    @pl.when(at_end)
    def _():
        pl.semaphore_signal(barrier, inc=1, device_id={"blk": opposite}, device_id_type=MESH)

    links = jnp.where(at_end, 1, 0) + jnp.where(inside(i + 1), 1, 0) + jnp.where(inside(i - 1), 1, 0)
    low[...] = jnp.full(low.shape, jnp.inf, jnp.float32)
    sec[...] = jnp.full(sec.shape, jnp.inf, jnp.float32)
    load.wait()
    pl.semaphore_wait(barrier, len(others) + links)

    def own_copy(way, c):
        step = 1 - 2 * way
        return pltpu.make_async_remote_copy(
            src_ref=x_ref.at[chunk(c)], dst_ref=buf.at[i, chunk(c)],
            send_sem=z_send.at[way, i, c], recv_sem=z_recv.at[i, c],
            device_id={"blk": i + step}, device_id_type=MESH,
        )

    def relay_copy(way, j, c):
        step = 1 - 2 * way
        return pltpu.make_async_remote_copy(
            src_ref=buf.at[j, chunk(c)], dst_ref=buf.at[j, chunk(c)],
            send_sem=z_send.at[way, j, c], recv_sem=z_recv.at[j, c],
            device_id={"blk": i + step}, device_id_type=MESH,
        )

    def far_copy(c):
        return pltpu.make_async_remote_copy(
            src_ref=x_ref.at[chunk(c)], dst_ref=buf.at[i, chunk(c)],
            send_sem=f_send.at[c], recv_sem=z_recv.at[i, c],
            device_id={"blk": opposite}, device_id_type=MESH,
        )

    for c in range(CH):
        for way in (0, 1):
            @pl.when(inside(i + 1 - 2 * way))
            def _():
                own_copy(way, c).start()

    @pl.when(at_end)
    def _():
        for c in range(CH):
            far_copy(c).start()

    mine_rows = rows_of(d, h)

    def query_copy(dd, hh):
        return pltpu.make_async_remote_copy(
            src_ref=x_ref, dst_ref=q.at[mine_rows],
            send_sem=q_send.at[dd * H + hh], recv_sem=q_recv.at[dd * H + hh],
            device_id=peer(dd, hh), device_id_type=MESH,
        )

    def query_relay(dd, hh):
        src_rows = rows_of(lax.rem(d + D - dd, D), h)
        return pltpu.make_async_remote_copy(
            src_ref=q.at[src_rows], dst_ref=q.at[src_rows],
            send_sem=q_send.at[dd * H + hh], recv_sem=q_recv.at[dd * H + hh],
            device_id=peer(0, hh), device_id_type=MESH,
        )

    for dd in range(1, D):
        query_copy(dd, 0).start()
    for hh in range(1, H):
        query_copy(0, hh).start()

    q[mine_rows, :] = x_ref[...]

    def each(steps, body):
        def over_steps(s, carry):
            def over_chunks(c, carry):
                def over_ways(way, carry):
                    body(s, c, way, i - s + 2 * s * way)
                    return carry

                return lax.fori_loop(0, 2, over_ways, carry)

            return lax.fori_loop(0, CH, over_chunks, carry)

        lax.fori_loop(1, 1 + steps, over_steps, 0)

    def passes(way, s, j):
        return inside(j) & inside(i + 1 - 2 * way) & (s + 1 < n - 1)

    def relay(s, c, way, j):
        @pl.when(passes(way, s, j) & (s < n))
        def _():
            copy = relay_copy(way, j, c)
            copy.wait_recv()
            copy.start()

    each(1, relay)

    for dd in range(1, D):
        query_copy(dd, 0).wait_recv()
        for hh in range(1, H):
            query_relay(dd, hh).start()
    for dd in range(D):
        for hh in range(1, H):
            query_copy(dd, hh).wait_recv()

    ones = jnp.ones((8, q.shape[1]), jnp.bfloat16)
    for t in range(D):
        wide = q[t * share : (t + 1) * share, :].astype(jnp.float32)
        square = wide * wide
        head = square.astype(jnp.bfloat16)
        tail = (square - head.astype(jnp.float32)).astype(jnp.bfloat16)
        qn[t] = nt_dot(ones, head) + nt_dot(ones, tail)

    def result_copy(k, dd, hh):
        return pltpu.make_async_remote_copy(
            src_ref=mine.at[k, lax.rem(d + dd, D)], dst_ref=inbox.at[k, dd * H + hh],
            send_sem=p_send.at[k, dd * H + hh], recv_sem=p_recv.at[k, dd * H + hh],
            device_id=peer(dd, hh), device_id_type=MESH,
        )

    def work(s, c, way, j):
        relay(s + 1, c, way, j - 1 + 2 * way)

        @pl.when(inside(j))
        def _():
            @pl.when(jnp.logical_not(passes(way, s, j)))
            def _():
                relay_copy(way, j, c).wait_recv()

            k = jnp.where(way == 0, s, n - s) - 1
            piece = buf[j, chunk(c), :]
            wide = piece.astype(jnp.float32)
            norms = jnp.sum(wide * wide, axis=1, keepdims=True)
            scaled = (wide * -2.0).astype(jnp.bfloat16)
            for t in range(Q // TQ):
                lanes = slice(t * TQ, (t + 1) * TQ)
                part = nt_dot(scaled, q[lanes, :]) + norms
                lo, se = low[k, :, lanes], sec[k, :, lanes]
                for r in range(CR // 8):
                    value = part[8 * r : 8 * r + 8]
                    se = jnp.minimum(se, jnp.maximum(lo, value))
                    lo = jnp.minimum(lo, value)
                low[k, :, lanes] = lo
                sec[k, :, lanes] = se

            @pl.when(c == CH - 1)
            def _():
                for t in range(D):
                    lanes = slice(t * share, (t + 1) * share)
                    lo, se = low[k, :, lanes], sec[k, :, lanes]
                    for turn in (4, 2, 1):
                        lo, se = combine(
                            lo, se, pltpu.roll(lo, turn, 0), pltpu.roll(se, turn, 0)
                        )
                    mine[k, t, 0:1, :] = lo[0:1]
                    mine[k, t, 1:2, :] = se[0:1]
                for dd, hh in reversed(others):
                    result_copy(k, dd, hh).start()

    each(n - 1, work)

    def finish(k, carry):
        lo, se = mine[k, d, 0:1, :], mine[k, d, 1:2, :]
        for dd, hh in others:
            result_copy(k, dd, hh).wait_recv()
            at = dd * H + hh
            lo, se = combine(lo, se, inbox[k, at, 0:1, :], inbox[k, at, 1:2, :])
        norms = qn[d, 0:1, :]
        best_ref[k] = lo
        second_ref[k] = se
        norm_ref[...] = norms
        return carry

    def sent_relay(s, c, way, j):
        @pl.when(passes(way, s, j))
        def _():
            relay_copy(way, j, c).wait_send()

    each(n - 1, sent_relay)
    for c in range(CH):
        for way in (0, 1):
            @pl.when(inside(i + 1 - 2 * way))
            def _():
                own_copy(way, c).wait_send()

    @pl.when(at_end)
    def _():
        for c in range(CH):
            far_copy(c).wait_send()

    for dd in range(1, D):
        query_copy(dd, 0).wait_send()
        for hh in range(1, H):
            query_relay(dd, hh).wait_send()
    for hh in range(1, H):
        query_copy(0, hh).wait_send()

    lax.fori_loop(0, n - 1, finish, 0)

    def sent_results(k, carry):
        for dd, hh in others:
            result_copy(k, dd, hh).wait_send()
        return carry

    lax.fori_loop(0, n - 1, sent_results, 0)


def solution(mesh):
    n, D, H = mesh.shape["blk"], mesh.shape["desc"], mesh.shape["half"]

    def per_device(descriptors):
        block = descriptors[0]
        R, depth = block.shape
        CH = 2 if R % 32 == 0 else 1
        share = H * R
        out = pltpu.VMEM((n - 1, 1, share), jnp.float32)
        vmem = pl.BlockSpec(memory_space=pltpu.VMEM)
        lo, se, norms = pl.pallas_call(
            functools.partial(kernel, n, D, H, CH),
            out_shape=(out, out, pltpu.VMEM((1, share), jnp.float32)),
            in_specs=[pl.BlockSpec(memory_space=pltpu.HBM)],
            out_specs=(vmem, vmem, vmem),
            scratch_shapes=[
                pltpu.VMEM((R, depth), jnp.bfloat16),
                pltpu.VMEM((n, R, depth), jnp.bfloat16),
                pltpu.VMEM((D * share, depth), jnp.bfloat16),
                pltpu.VMEM((D, 8, share), jnp.float32),
                pltpu.VMEM((n - 1, 8, D * share), jnp.float32),
                pltpu.VMEM((n - 1, 8, D * share), jnp.float32),
                pltpu.VMEM((n - 1, D, 2, share), jnp.float32),
                pltpu.VMEM((n - 1, D * H, 2, share), jnp.float32),
                pltpu.SemaphoreType.DMA,
                pltpu.SemaphoreType.DMA((CH,)),
                pltpu.SemaphoreType.DMA((2, n, CH)),
                pltpu.SemaphoreType.DMA((n, CH)),
                pltpu.SemaphoreType.DMA((D * H,)),
                pltpu.SemaphoreType.DMA((D * H,)),
                pltpu.SemaphoreType.DMA((n - 1, D * H)),
                pltpu.SemaphoreType.DMA((n - 1, D * H)),
            ],
            compiler_params=pltpu.CompilerParams(collective_id=0, has_side_effects=True),
        )(block)
        return norms + lo, norms + se

    in_specs = (P(("groups", "blk"), ("desc", "half"), None),)
    out_specs = (P(None, ("groups", "blk"), "desc"), P(None, ("groups", "blk"), "desc"))
    return jax.shard_map(
        per_device, mesh=mesh, in_specs=in_specs, out_specs=out_specs, check_vma=False
    )
```
